32 devices in a mesh: dom: 4 (over z), feat: 8 (over y, x, core).
Axes of the slice: x: 2, y: 2, z: 4, core: 2. Of those that a mesh axis runs over, the one named last changes fastest.
Arguments:
- node_feats: bfloat16 [4096, 512], P('dom', 'feat'), may hold values from -6 to 6
- rel_weight: bfloat16 [4, 512, 512], replicated, may hold values from -0.25 to 0.25
- self_weight: bfloat16 [512, 512], replicated, may hold values from -0.25 to 0.25
- bias: float32 [512], replicated, may hold values from -3 to 3
- out_degree: int32 [4, 4096], P(None, 'dom'), may hold values from 0 to 63
- adjacency: int32 [4, 8, 64, 256, 256], P('dom', 'feat'), may hold values 0 or 1
- tile_index: int32 [4, 8, 64, 3], P('dom', 'feat'), may hold values from 0 to 15, as said below
- tile_count: int32 [4, 8], P('dom', 'feat'), may hold values from 1 to 64, as said below
Outputs:
- embedding: bfloat16 [4096, 512], P('dom', 'feat')
The draws below stay inside these ranges and needn't reach their ends.
Inputs may be any that keep to these rules, and one draw needn't show every extreme that they name: `tile_index`: the three entries of a slot are a relation below 4, a destination block below 16 and a source block of the device's own group below 4; entries of slots beyond a device's count are arbitrary within the range. `tile_count`: some device holds exactly 64 live slots.
All inputs are finite; a program needn't handle non-finite values. No bound on the sum of `adjacency` on one device may be relied on, other than what follows from the above.
Results may differ from the reference program's by a relative error of at most 0.0049.
Values may be sent and summed in bfloat16 or wider, within the bound.
No kernel may reach another device: no remote copies, remote signals or barrier semaphores. Data moves between devices by JAX's collectives and lax.ppermute only.
A program may use at most 128 MiB of HBM per device.

```python
import jax
import jax.numpy as jnp
from jax import lax

H = 512
R = 4
TILE_SIZE = 256
BG = 4
TILE_DEV = 64
NODES = 4096
N_DOM = 4
N_FEAT = 8


def draw_tile_index(key, part):
    first, second, third = jax.random.split(jax.random.fold_in(key, 11), 3)
    shape = (N_DOM, N_FEAT, TILE_DEV)
    relation = jax.random.randint(first, shape, 0, R)
    target = jax.random.randint(second, shape, 0, N_DOM * BG)
    source = jax.random.randint(third, shape, 0, BG)
    return jnp.stack([relation, target, source], axis=-1).astype(jnp.int32)


def draw_tile_count(key, part):
    first, second = jax.random.split(jax.random.fold_in(key, 23), 2)
    counts = jax.random.randint(first, (N_DOM * N_FEAT,), 1, TILE_DEV + 1)
    position = jax.random.randint(second, (), 0, N_DOM * N_FEAT)
    positions = jnp.arange(N_DOM * N_FEAT)
    counts = jnp.where(positions == position, TILE_DEV, counts)
    return counts.reshape(N_DOM, N_FEAT).astype(jnp.int32)


def touch_ends(result, stream_key, low, largest):
    spot = [jax.random.randint(jax.random.fold_in(stream_key, axis), (), 0, length) for axis, length in enumerate(result.shape)]
    longest = result.shape.index(max(result.shape))
    next_to = spot[:longest] + [(spot[longest] + 1) % result.shape[longest]] + spot[longest + 1:]
    return result.at[tuple(spot)].set(low).at[tuple(next_to)].set(largest)


def block_levels(stream_key, shape, cuts, low, largest):
    factor_of, own = 1.0, jax.random.fold_in(stream_key, 6)
    for axis_at, blocks in cuts:
        heights = jnp.exp(jax.random.uniform(jax.random.fold_in(own, axis_at), (blocks,), jnp.float32, low / len(cuts), largest / len(cuts)))
        factor_of = factor_of * jnp.repeat(heights, shape[axis_at] // blocks).reshape([-1 if axis == axis_at else 1 for axis in range(len(shape))])
    return factor_of


def noise(stream_key, extent, spread, reach, pieces=(), kind=jnp.bfloat16):
    array = spread * jax.random.normal(stream_key, extent, jnp.float32)
    if pieces:
        array = array * block_levels(stream_key, extent, pieces, -0.22, 0.18)
    return jnp.clip(array, -reach, reach).astype(kind)


def setup_inputs(seed: int = 0) -> dict:
    key_of = jax.random.split(jax.random.key(seed), 9)
    node_feats = noise(key_of[0], (NODES, H), 1.0, 6.0, ((0, 4), (1, 8)))
    rel_weight = noise(key_of[1], (R, H, H), H ** -0.5, 0.25)
    self_weight = noise(key_of[2], (H, H), H ** -0.5, 0.25)
    bias = noise(key_of[3], (H,), 0.5, 3.0, (), jnp.float32)
    out_degree = touch_ends(jax.random.randint(key_of[4], (R, NODES), 0, 64), jax.random.fold_in(key_of[4], 1), 0, 63).astype(jnp.int32)
    adjacency = touch_ends((jax.random.randint(key_of[5], (N_DOM, N_FEAT, TILE_DEV, TILE_SIZE, TILE_SIZE), 0, 8) < 1).astype(jnp.int32), jax.random.fold_in(key_of[5], 1), 0, 1)
    tile_index = draw_tile_index(jax.random.fold_in(key_of[8], 71), 0)
    tile_count = draw_tile_count(jax.random.fold_in(key_of[8], 71), 0)
    return dict(node_feats=node_feats, rel_weight=rel_weight, self_weight=self_weight, bias=bias, out_degree=out_degree, adjacency=adjacency, tile_index=tile_index, tile_count=tile_count)


def reference(node_feats, rel_weight, self_weight, bias, out_degree, adjacency, tile_index, tile_count):
    inv_degree = 1.0 / jnp.maximum(out_degree, 1).astype(jnp.float32)

    def transform(relation):
        product = jnp.dot(node_feats, rel_weight[relation], preferred_element_type=jnp.float32)
        return (product * inv_degree[relation][:, None]).astype(jnp.bfloat16)

    messages = lax.map(transform, jnp.arange(R, dtype=jnp.int32))
    flat_tiles = adjacency.reshape(-1, TILE_SIZE, TILE_SIZE)
    flat_index = tile_index.reshape(-1, 3).astype(jnp.int32)
    slot_ids = jnp.arange(TILE_DEV, dtype=jnp.int32)
    live_mask = (slot_ids[None, None, :] < tile_count[:, :, None]).reshape(-1).astype(jnp.float32)
    group_ids = jnp.repeat(jnp.arange(N_DOM, dtype=jnp.int32), N_FEAT * TILE_DEV)

    def accumulate(running, items):
        tile_cells, entry, weight, group = items
        source_row = ((group * BG + entry[2]) * TILE_SIZE).astype(jnp.int32)
        target_row = (entry[1] * TILE_SIZE).astype(jnp.int32)
        source_msg = lax.dynamic_slice(messages, (entry[0].astype(jnp.int32), source_row, jnp.int32(0)), (1, TILE_SIZE, H))[0]
        contribution = jnp.dot(tile_cells.astype(jnp.bfloat16), source_msg, preferred_element_type=jnp.float32) * weight
        current = lax.dynamic_slice_in_dim(running, target_row, TILE_SIZE, 0)
        return lax.dynamic_update_slice_in_dim(running, current + contribution, target_row, 0), None

    start = jnp.zeros((NODES, H), jnp.float32)
    aggregate, unused = lax.scan(accumulate, start, (flat_tiles, flat_index, live_mask, group_ids))
    self_term = jnp.dot(node_feats, self_weight, preferred_element_type=jnp.float32)
    return (aggregate + self_term + bias[None, :]).astype(jnp.bfloat16)
```

```python
import functools

import jax
import jax.numpy as jnp
from jax import lax
from jax.experimental import pallas as pl
from jax.experimental.pallas import tpu as pltpu
from jax.sharding import PartitionSpec as P

RING = 8


def message_kernel(
    place_ref, order_ref, blocks_ref, weight_ref, self_ref, bias_ref, degree_ref, msg_ref, own_ref, feats
):
    block_count, block_rows, _ = blocks_ref.shape
    for step in range(block_count):
        row = pl.multiple_of(order_ref[step] * block_rows, block_rows)
        feats[pl.ds(row, block_rows), :] = blocks_ref[step]
    tile = min(256, feats.shape[1])
    for relation in range(weight_ref.shape[0]):
        inv_degree = 1.0 / jnp.maximum(degree_ref[relation], 1).astype(jnp.float32)
        for start in range(0, feats.shape[1], tile):
            product = jnp.dot(
                weight_ref[relation], feats[:, start : start + tile], preferred_element_type=jnp.float32
            )
            scale = inv_degree[None, start : start + tile]
            msg_ref[relation, :, start : start + tile] = (product * scale).astype(jnp.bfloat16)
    own_ref[...] = (
        jnp.dot(self_ref[...], feats[...], preferred_element_type=jnp.float32) + bias_ref[...]
    )


def tile_kernel(group_blocks, place_ref, index_ref, tiles_ref, msg_ref, keep_ref, send_ref, picked, ring, total, sems):
    tile = tiles_ref.shape[-1]
    width = keep_ref.shape[0]
    group, live, core = place_ref[0], place_ref[1], place_ref[2]
    first = group * group_blocks
    total[...] = jnp.zeros_like(total)

    def pick(slot, found):
        target = index_ref[3 * slot + 1] - first
        inside = jnp.logical_and(target >= 0, target < group_blocks)

        @pl.when(inside)
        def _():
            picked[found] = slot

        return found + inside.astype(jnp.int32)

    found = lax.fori_loop(0, live, pick, jnp.int32(0))

    def fetch(step):
        place = lax.rem(step, RING)
        return pltpu.make_async_copy(tiles_ref.at[picked[step]], ring.at[place], sems.at[place])

    for step in range(RING):

        @pl.when(step < found)
        def _():
            fetch(step).start()

    def work(step, carry):
        slot = picked[step]
        relation = index_ref[3 * slot]
        target = pl.multiple_of((index_ref[3 * slot + 1] - first) * tile, tile)
        source = pl.multiple_of(index_ref[3 * slot + 2] * tile, tile)
        fetch(step).wait()
        cells = ring[lax.rem(step, RING)].astype(jnp.float32).astype(jnp.bfloat16)
        part = lax.dot_general(
            msg_ref[relation, :, pl.ds(source, tile)],
            cells,
            (((1,), (1,)), ((), ())),
            preferred_element_type=jnp.float32,
        )
        total[:, pl.ds(target, tile)] += part

        @pl.when(step + RING < found)
        def _():
            fetch(step + RING).start()

        return carry

    lax.fori_loop(0, found, work, 0)
    keep_row = pl.multiple_of(core * width, width)
    send_row = pl.multiple_of((1 - core) * width, width)
    keep_ref[...] = total[pl.ds(keep_row, width), :].astype(jnp.bfloat16)
    send_ref[...] = total[pl.ds(send_row, width), :].astype(jnp.bfloat16)


def body(node_feats, rel_weight, self_weight, bias, out_degree, adjacency, tile_index, tile_count):
    rows, columns = node_feats.shape
    relations, hidden = rel_weight.shape[:2]
    slots, tile = adjacency.shape[2], adjacency.shape[-1]
    group_blocks = rows // tile
    feat_count, dom_count = lax.axis_size("feat"), lax.axis_size("dom")
    levels = feat_count.bit_length() - 1
    feat, dom = lax.axis_index("feat"), lax.axis_index("dom")
    core = feat % 2
    half = hidden // 2
    vmem = pl.BlockSpec(memory_space=pltpu.VMEM)
    smem = pl.BlockSpec(memory_space=pltpu.SMEM)

    def swap(value, mask):
        return lax.ppermute(value, "feat", [(i, i ^ mask) for i in range(feat_count)])

    block = node_feats.T
    near = [block] + [swap(block, mask) for mask in range(2, feat_count, 2)]
    near = jnp.stack(near)
    far = swap(near, 1)
    blocks = jnp.concatenate([near, far])
    order = jnp.array([m for m in range(0, feat_count, 2)] + [m + 1 for m in range(0, feat_count, 2)])
    order = (feat ^ order).astype(jnp.int32)
    weight_t = rel_weight.reshape(relations, hidden, feat_count // 2, 2, columns)
    weight_t = weight_t.transpose(0, 3, 2, 4, 1).reshape(relations, hidden, hidden)
    self_t = lax.dynamic_slice_in_dim(self_weight, feat * columns, columns, 1).T
    bias_t = lax.dynamic_slice_in_dim(bias, feat * columns, columns, 0)[:, None]
    messages, own = pl.pallas_call(
        message_kernel,
        out_shape=(
            jax.ShapeDtypeStruct((relations, hidden, rows), jnp.bfloat16),
            jax.ShapeDtypeStruct((columns, rows), jnp.float32),
        ),
        in_specs=[smem, smem, vmem, vmem, vmem, vmem, vmem],
        out_specs=(vmem, vmem),
        scratch_shapes=[pltpu.VMEM((hidden, rows), jnp.bfloat16)],
        compiler_params=pltpu.CompilerParams(vmem_limit_bytes=32 * 2**20),
        cost_estimate=pl.CostEstimate(
            flops=2 * relations * hidden * hidden * rows, bytes_accessed=8 * 2**20, transcendentals=0
        ),
        name="messages",
    )(jnp.zeros((1,), jnp.int32), order, blocks, weight_t, self_t, bias_t, out_degree)

    live = tile_count[0, 0]
    index = tile_index.reshape(-1)
    tiles = adjacency[0, 0]

    def partial_sums(group):
        place = jnp.stack([group, live, core]).astype(jnp.int32)
        shape = jax.ShapeDtypeStruct((half, rows), jnp.bfloat16)
        return pl.pallas_call(
            functools.partial(tile_kernel, group_blocks),
            out_shape=(shape, shape),
            in_specs=[smem, smem, pl.BlockSpec(memory_space=pl.ANY), vmem],
            out_specs=(vmem, vmem),
            scratch_shapes=[
                pltpu.SMEM((slots,), jnp.int32),
                pltpu.VMEM((RING, tile, tile), jnp.int32),
                pltpu.VMEM((hidden, rows), jnp.float32),
                pltpu.SemaphoreType.DMA((RING,)),
            ],
            compiler_params=pltpu.CompilerParams(vmem_limit_bytes=24 * 2**20),
            cost_estimate=pl.CostEstimate(
                flops=2 * tile * tile * hidden * slots // dom_count,
                bytes_accessed=4 * tile * tile * slots // dom_count,
                transcendentals=0,
            ),
            name="tiles",
        )(place, index, tiles, messages)

    def total_of(parts):
        return functools.reduce(jnp.add, [part.astype(jnp.float32) for part in parts])

    def pick(value, level, bit):
        axis = value.ndim - 2 - level
        return lax.dynamic_index_in_dim(value, bit, axis, keepdims=True)

    def reduce_group(keep, send):
        grid = (2,) * (levels - 1) + (columns, rows)
        arrived = swap(send, 1)
        parts = [keep.reshape(grid), arrived.reshape(grid)]
        results = []
        for way in range(2):
            part = rows // 2
            mine = [p[..., way * part : (way + 1) * part] for p in parts]
            orders = list(range(1, levels))
            for level in orders if way == 0 else orders[::-1]:
                bit = (feat >> level) & 1
                away = total_of([pick(p, level, 1 - bit) for p in mine]).astype(jnp.bfloat16)
                mine = [pick(p, level, bit) for p in mine] + [swap(away, 1 << level)]
            results.append(total_of(mine).reshape(columns, part))
        return jnp.concatenate(results, axis=1)

    arrivals = []
    for step in list(range(1, dom_count)) + [0]:
        shares = reduce_group(*partial_sums((dom + step) % dom_count))
        if step:
            ring = [(i, (i + step) % dom_count) for i in range(dom_count)]
            shares = lax.ppermute(shares.astype(jnp.bfloat16), "dom", ring)
        arrivals.append(shares)
    return (total_of(arrivals) + own).astype(jnp.bfloat16).T


def solution(mesh):
    placed = (
        P("dom", "feat"),
        P(),
        P(),
        P(),
        P(None, "dom"),
        P("dom", "feat", None, None, None),
        P("dom", "feat", None, None),
        P("dom", "feat"),
    )
    return jax.shard_map(
        body, mesh=mesh, in_specs=placed, out_specs=P("dom", "feat"), check_vma=False
    )
```

```python
import functools

import jax
import jax.numpy as jnp
from jax import lax
from jax.experimental import pallas as pl
from jax.experimental.pallas import tpu as pltpu
from jax.sharding import PartitionSpec as P

RING = 8


def message_kernel(order_ref, near_ref, far_ref, weight_ref, self_ref, bias_ref, degree_ref, msg_ref, own_ref, feats):
    block_count, block_rows, _ = near_ref.shape
    for step in range(block_count):
        for side, blocks in enumerate((near_ref, far_ref)):
            place = order_ref[side * block_count + step] * block_rows
            feats[pl.ds(pl.multiple_of(place, block_rows), block_rows), :] = blocks[step]
    tile = min(256, feats.shape[1])
    for relation in range(weight_ref.shape[0]):
        inv_degree = 1.0 / jnp.maximum(degree_ref[relation], 1).astype(jnp.float32)
        for start in range(0, feats.shape[1], tile):
            product = jnp.dot(
                weight_ref[relation], feats[:, start : start + tile], preferred_element_type=jnp.float32
            )
            scale = inv_degree[None, start : start + tile]
            msg_ref[relation, :, start : start + tile] = (product * scale).astype(jnp.bfloat16)
    own_ref[...] = (
        jnp.dot(self_ref[...], feats[...], preferred_element_type=jnp.float32) + bias_ref[...]
    )


def tile_kernel(
    group_blocks, columns, place_ref, index_ref, after_ref, tiles_ref, msg_ref, keep_ref, send_ref, done_ref, picked, ring, total, sems
):
    tile = tiles_ref.shape[-1]
    live, core = place_ref[0], place_ref[1]
    done_ref[0] = after_ref[0]

    def fetch(step):
        place = lax.rem(step, RING)
        return pltpu.make_async_copy(tiles_ref.at[picked[0, step]], ring.at[place], sems.at[place])

    def pick(slot, found):
        target = index_ref[3 * slot + 1]
        block = jnp.int32(-1)
        for number in range(place_ref.shape[0] - 2):
            local = target - place_ref[2 + number] * group_blocks
            inside = jnp.logical_and(local >= 0, local < group_blocks)
            block = jnp.where(inside, local + number * group_blocks, block)

        @pl.when(block >= 0)
        def _():
            picked[0, found] = slot
            picked[1, found] = block * tile

            @pl.when(found < RING)
            def _():
                fetch(found).start()

        return found + (block >= 0).astype(jnp.int32)

    found = lax.fori_loop(0, live, pick, jnp.int32(0))
    picked[0, found] = 0
    picked[1, found] = 0
    total[...] = jnp.zeros_like(total)

    def product(step, cells):
        slot = picked[0, step]
        source = pl.multiple_of(index_ref[3 * slot + 2] * tile, tile)
        return lax.dot_general(
            msg_ref[index_ref[3 * slot], :, pl.ds(source, tile)],
            cells.astype(jnp.float32).astype(jnp.bfloat16),
            (((1,), (1,)), ((), ())),
            preferred_element_type=jnp.float32,
        )

    def work(pair, carry):
        one, two = 2 * pair, 2 * pair + 1
        fetch(one).wait()

        @pl.when(two < found)
        def _():
            fetch(two).wait()

        first = product(one, ring[lax.rem(one, RING)])
        second = product(two, jnp.where(two < found, ring[lax.rem(two, RING)], 0))
        total[:, pl.ds(pl.multiple_of(picked[1, one], tile), tile)] += first
        total[:, pl.ds(pl.multiple_of(picked[1, two], tile), tile)] += second
        for step in (one + RING, two + RING):

            @pl.when(step < found)
            def _():
                fetch(step).start()

        return carry

    lax.fori_loop(0, (found + 1) // 2, work, 0)
    for number in range(keep_ref.shape[0] // columns):
        rows = pl.ds(number * columns, columns)
        for ref, side in ((keep_ref, core), (send_ref, 1 - core)):
            start = pl.multiple_of((2 * number + side) * columns, columns)
            ref[rows, :] = total[pl.ds(start, columns), :].astype(jnp.bfloat16)


def body(node_feats, rel_weight, self_weight, bias, out_degree, adjacency, tile_index, tile_count):
    rows, columns = node_feats.shape
    relations, hidden = rel_weight.shape[:2]
    slots, tile = adjacency.shape[2], adjacency.shape[-1]
    group_blocks = rows // tile
    feat_count, dom_count = lax.axis_size("feat"), lax.axis_size("dom")
    levels = feat_count.bit_length() - 1
    feat, dom = lax.axis_index("feat"), lax.axis_index("dom")
    core = feat % 2
    half = hidden // 2
    vmem = pl.BlockSpec(memory_space=pltpu.VMEM)
    smem = pl.BlockSpec(memory_space=pltpu.SMEM)

    def swap(value, mask):
        return lax.ppermute(value, "feat", [(i, i ^ mask) for i in range(feat_count)])

    block = node_feats.T
    near = [block] + [swap(block, mask) for mask in range(2, feat_count, 2)]
    near = jnp.stack(near)
    far = swap(near, 1)
    order = jnp.array([m for m in range(0, feat_count, 2)] + [m + 1 for m in range(0, feat_count, 2)])
    order = (feat ^ order).astype(jnp.int32)
    weight_t = rel_weight.transpose(0, 2, 1)
    self_t = lax.dynamic_slice_in_dim(self_weight, feat * columns, columns, 1).T
    bias_t = lax.dynamic_slice_in_dim(bias, feat * columns, columns, 0)[:, None]
    messages, own = pl.pallas_call(
        message_kernel,
        out_shape=(
            jax.ShapeDtypeStruct((relations, hidden, rows), jnp.bfloat16),
            jax.ShapeDtypeStruct((columns, rows), jnp.float32),
        ),
        in_specs=[smem] + [vmem] * 6,
        out_specs=(vmem, vmem),
        scratch_shapes=[pltpu.VMEM((hidden, rows), jnp.bfloat16)],
        compiler_params=pltpu.CompilerParams(vmem_limit_bytes=32 * 2**20),
        cost_estimate=pl.CostEstimate(
            flops=2 * relations * hidden * hidden * rows, bytes_accessed=8 * 2**20, transcendentals=0
        ),
        name="messages",
    )(order, near, far, weight_t, self_t, bias_t, out_degree)

    live = tile_count[0, 0]
    index = tile_index.reshape(-1)
    tiles = adjacency[0, 0]

    def partial_sums(steps, after):
        groups = [(dom + step) % dom_count for step in steps]
        place = jnp.stack([live, core] + groups).astype(jnp.int32)
        width = len(steps) * rows
        shape = jax.ShapeDtypeStruct((half, width), jnp.bfloat16)
        return pl.pallas_call(
            functools.partial(tile_kernel, group_blocks, columns),
            out_shape=(shape, shape, jax.ShapeDtypeStruct((1,), jnp.int32)),
            in_specs=[smem, smem, smem, pl.BlockSpec(memory_space=pltpu.HBM), vmem],
            out_specs=(vmem, vmem, smem),
            scratch_shapes=[
                pltpu.SMEM((2, slots + 1), jnp.int32),
                pltpu.VMEM((RING, tile, tile), jnp.int32),
                pltpu.VMEM((hidden, width), jnp.float32),
                pltpu.SemaphoreType.DMA((RING,)),
            ],
            compiler_params=pltpu.CompilerParams(vmem_limit_bytes=40 * 2**20),
            cost_estimate=pl.CostEstimate(
                flops=2 * tile * tile * hidden * slots * len(steps) // dom_count,
                bytes_accessed=4 * tile * tile * slots * len(steps) // dom_count,
                transcendentals=0,
            ),
            name="tiles",
        )(place, index, after, tiles, messages)

    def total_of(parts):
        return functools.reduce(jnp.add, [part.astype(jnp.float32) for part in parts])

    def pick(value, level, bit):
        axis = value.ndim - 2 - level
        return lax.dynamic_index_in_dim(value, bit, axis, keepdims=True)

    def reduce_group(keep, send):
        grid = (2,) * (levels - 1) + (columns, keep.shape[1])
        arrived = swap(send, 1)
        parts = [keep.reshape(grid), arrived.reshape(grid)]
        results = []
        for way in range(2):
            part = keep.shape[1] // 2
            mine = [p[..., way * part : (way + 1) * part] for p in parts]
            orders = list(range(1, levels))
            for level in orders if way == 0 else orders[::-1]:
                bit = (feat >> level) & 1
                away = total_of([pick(p, level, 1 - bit) for p in mine]).astype(jnp.bfloat16)
                mine = [pick(p, level, bit) for p in mine] + [swap(away, 1 << level)]
            results.append(total_of(mine).reshape(columns, part))
        return jnp.concatenate(results, axis=1)

    arrivals = []
    after = jnp.zeros((1,), jnp.int32)
    for steps in (list(range(1, dom_count)), [0]):
        keep, send, after = partial_sums(steps, after)
        shares = reduce_group(keep, send)
        for number, step in enumerate(steps):
            share = shares[:, number * rows : (number + 1) * rows]
            if step:
                ring = [(i, (i + step) % dom_count) for i in range(dom_count)]
                share = lax.ppermute(share.astype(jnp.bfloat16), "dom", ring)
            arrivals.append(share)
    return (total_of(arrivals) + own).astype(jnp.bfloat16).T


def solution(mesh):
    placed = (
        P("dom", "feat"),
        P(),
        P(),
        P(),
        P(None, "dom"),
        P("dom", "feat", None, None, None),
        P("dom", "feat", None, None),
        P("dom", "feat"),
    )
    return jax.shard_map(
        body, mesh=mesh, in_specs=placed, out_specs=P("dom", "feat"), check_vma=False
    )
```

```python
import functools

import jax
import jax.numpy as jnp
from jax import lax
from jax.experimental import pallas as pl
from jax.experimental.pallas import tpu as pltpu
from jax.sharding import PartitionSpec as P


RING = 8


def CHUNKS(dom_count):
    return list(range(1, dom_count)), [0]


def message_kernel(order_ref, near_ref, far_ref, weight_ref, self_ref, bias_ref, degree_ref, msg_ref, own_ref, feats):
    block_count, block_rows, _ = near_ref.shape
    for step in range(block_count):
        for side, blocks in enumerate((near_ref, far_ref)):
            place = order_ref[side * block_count + step] * block_rows
            feats[pl.ds(pl.multiple_of(place, block_rows), block_rows), :] = blocks[step]
    tile = min(256, feats.shape[1])
    for relation in range(weight_ref.shape[0]):
        inv_degree = 1.0 / jnp.maximum(degree_ref[relation], 1).astype(jnp.float32)
        for start in range(0, feats.shape[1], tile):
            product = jnp.dot(
                weight_ref[relation], feats[:, start : start + tile], preferred_element_type=jnp.float32
            )
            scale = inv_degree[None, start : start + tile]
            msg_ref[relation, :, start : start + tile] = (product * scale).astype(jnp.bfloat16)
    own_ref[...] = (
        jnp.dot(self_ref[...], feats[...], preferred_element_type=jnp.float32) + bias_ref[...]
    )


def tile_kernel(
    group_blocks, columns, place_ref, index_ref, after_ref, tiles_ref, msg_ref, keep_ref, send_ref, done_ref, picked, ring, total, sems
):
    tile = tiles_ref.shape[-1]
    live, core = place_ref[0], place_ref[1]
    done_ref[0] = after_ref[0]

    def fetch(step):
        place = lax.rem(step, RING)
        return pltpu.make_async_copy(tiles_ref.at[picked[0, step]], ring.at[place], sems.at[place])

    def pick(slot, found):
        target = index_ref[3 * slot + 1]
        block = jnp.int32(-1)
        for number in range(place_ref.shape[0] - 2):
            local = target - place_ref[2 + number] * group_blocks
            inside = jnp.logical_and(local >= 0, local < group_blocks)
            block = jnp.where(inside, local + number * group_blocks, block)

        @pl.when(block >= 0)
        def _():
            picked[0, found] = slot
            picked[1, found] = block * tile

            @pl.when(found < RING)
            def _():
                fetch(found).start()

        return found + (block >= 0).astype(jnp.int32)

    found = lax.fori_loop(0, live, pick, jnp.int32(0))
    picked[0, found] = 0
    picked[1, found] = 0
    total[...] = jnp.zeros_like(total)

    def product(step, cells):
        slot = picked[0, step]
        source = pl.multiple_of(index_ref[3 * slot + 2] * tile, tile)
        return lax.dot_general(
            msg_ref[index_ref[3 * slot], :, pl.ds(source, tile)],
            cells.astype(jnp.float32).astype(jnp.bfloat16),
            (((1,), (1,)), ((), ())),
            preferred_element_type=jnp.float32,
        )

    def work(pair, carry):
        one, two = 2 * pair, 2 * pair + 1
        fetch(one).wait()

        @pl.when(two < found)
        def _():
            fetch(two).wait()

        first = product(one, ring[lax.rem(one, RING)])
        second = product(two, jnp.where(two < found, ring[lax.rem(two, RING)], 0))
        total[:, pl.ds(pl.multiple_of(picked[1, one], tile), tile)] += first
        total[:, pl.ds(pl.multiple_of(picked[1, two], tile), tile)] += second
        for step in (one + RING, two + RING):

            @pl.when(step < found)
            def _():
                fetch(step).start()

        return carry

    lax.fori_loop(0, (found + 1) // 2, work, 0)
    for number in range(keep_ref.shape[0] // columns):
        rows = pl.ds(number * columns, columns)
        for ref, side in ((keep_ref, core), (send_ref, 1 - core)):
            start = pl.multiple_of((2 * number + side) * columns, columns)
            ref[rows, :] = total[pl.ds(start, columns), :].astype(jnp.bfloat16)


def body(node_feats, rel_weight, self_weight, bias, out_degree, adjacency, tile_index, tile_count):
    rows, columns = node_feats.shape
    relations, hidden = rel_weight.shape[:2]
    slots, tile = adjacency.shape[2], adjacency.shape[-1]
    group_blocks = rows // tile
    feat_count, dom_count = lax.axis_size("feat"), lax.axis_size("dom")
    levels = feat_count.bit_length() - 1
    feat, dom = lax.axis_index("feat"), lax.axis_index("dom")
    core = feat % 2
    half = hidden // 2
    vmem = pl.BlockSpec(memory_space=pltpu.VMEM)
    smem = pl.BlockSpec(memory_space=pltpu.SMEM)

    def swap(value, mask):
        return lax.ppermute(value, "feat", [(i, i ^ mask) for i in range(feat_count)])

    block = node_feats.T
    near = [block] + [swap(block, mask) for mask in range(2, feat_count, 2)]
    near = jnp.stack(near)
    far = swap(near, 1)
    order = jnp.array([m for m in range(0, feat_count, 2)] + [m + 1 for m in range(0, feat_count, 2)])
    order = (feat ^ order).astype(jnp.int32)
    weight_t = rel_weight.transpose(0, 2, 1)
    self_t = lax.dynamic_slice_in_dim(self_weight, feat * columns, columns, 1).T
    bias_t = lax.dynamic_slice_in_dim(bias, feat * columns, columns, 0)[:, None]
    messages, own = pl.pallas_call(
        message_kernel,
        out_shape=(
            jax.ShapeDtypeStruct((relations, hidden, rows), jnp.bfloat16),
            jax.ShapeDtypeStruct((columns, rows), jnp.float32),
        ),
        in_specs=[smem] + [vmem] * 6,
        out_specs=(vmem, vmem),
        scratch_shapes=[pltpu.VMEM((hidden, rows), jnp.bfloat16)],
        compiler_params=pltpu.CompilerParams(vmem_limit_bytes=32 * 2**20),
        cost_estimate=pl.CostEstimate(
            flops=2 * relations * hidden * hidden * rows, bytes_accessed=8 * 2**20, transcendentals=0
        ),
        name="messages",
    )(order, near, far, weight_t, self_t, bias_t, out_degree)

    live = tile_count[0, 0]
    index = tile_index.reshape(-1)
    tiles = adjacency[0, 0]

    def partial_sums(steps, after):
        groups = [(dom + step) % dom_count for step in steps]
        place = jnp.stack([live, core] + groups).astype(jnp.int32)
        width = len(steps) * rows
        shape = jax.ShapeDtypeStruct((half, width), jnp.bfloat16)
        return pl.pallas_call(
            functools.partial(tile_kernel, group_blocks, columns),
            out_shape=(shape, shape, jax.ShapeDtypeStruct((1,), jnp.int32)),
            in_specs=[smem, smem, smem, pl.BlockSpec(memory_space=pltpu.HBM), vmem],
            out_specs=(vmem, vmem, smem),
            scratch_shapes=[
                pltpu.SMEM((2, slots + 1), jnp.int32),
                pltpu.VMEM((RING, tile, tile), jnp.int32),
                pltpu.VMEM((hidden, width), jnp.float32),
                pltpu.SemaphoreType.DMA((RING,)),
            ],
            compiler_params=pltpu.CompilerParams(vmem_limit_bytes=40 * 2**20),
            cost_estimate=pl.CostEstimate(
                flops=2 * tile * tile * hidden * slots * len(steps) // dom_count,
                bytes_accessed=4 * tile * tile * slots * len(steps) // dom_count,
                transcendentals=0,
            ),
            name="tiles",
        )(place, index, after, tiles, messages)

    def total_of(parts):
        return functools.reduce(jnp.add, [part.astype(jnp.float32) for part in parts])

    def pick(value, level, bit):
        axis = value.ndim - 2 - level
        return lax.dynamic_index_in_dim(value, bit, axis, keepdims=True)

    def reduce_group(keep, send):
        grid = (2,) * (levels - 1) + (columns, keep.shape[1])
        arrived = swap(send, 1)
        parts = [keep.reshape(grid), arrived.reshape(grid)]
        results = []
        for way in range(2):
            part = keep.shape[1] // 2
            mine = [p[..., way * part : (way + 1) * part] for p in parts]
            orders = list(range(1, levels))
            for level in orders if way == 0 else orders[::-1]:
                bit = (feat >> level) & 1
                away = total_of([pick(p, level, 1 - bit) for p in mine]).astype(jnp.bfloat16)
                came = swap(away, 1 << level)
                mine = [pick(p, level, bit) for p in mine] + [came]
            results.append(total_of(mine).reshape(columns, part))
        return jnp.concatenate(results, axis=1)

    arrivals = []
    after = jnp.zeros((1,), jnp.int32)
    for steps in CHUNKS(dom_count):
        keep, send, after = partial_sums(steps, after)
        shares = reduce_group(keep, send)
        for number, step in enumerate(steps):
            share = shares[:, number * rows : (number + 1) * rows]
            if step:
                ring = [(i, (i + step) % dom_count) for i in range(dom_count)]
                share = lax.ppermute(share.astype(jnp.bfloat16), "dom", ring)
            arrivals.append(share)
    return (total_of(arrivals) + own).astype(jnp.bfloat16).T


def solution(mesh):
    placed = (
        P("dom", "feat"),
        P(),
        P(),
        P(),
        P(None, "dom"),
        P("dom", "feat", None, None, None),
        P("dom", "feat", None, None),
        P("dom", "feat"),
    )
    return jax.shard_map(
        body, mesh=mesh, in_specs=placed, out_specs=P("dom", "feat"), check_vma=False
    )
```
